32 devices in a mesh: data: 1 (over z), seq: 32 (over y, x, core).
Axes of the slice: x: 4, y: 4, z: 1, core: 2. Of those that a mesh axis runs over, the one named last changes fastest.
The devices are a block of a 4x4x8 slice.
Arguments:
- x: bfloat16 [8192, 4096], P(('data', 'seq'))
- g: float32 [4096], replicated
- wqkv: bfloat16 [4096, 3, 32, 128], replicated
- wo: bfloat16 [32, 128, 4096], replicated
Outputs:
- output: bfloat16 [8192, 4096], P(('data', 'seq'))
All inputs are finite; a program needn't handle non-finite values.
Results may differ from the reference program's by a relative error of at most 0.0030117.
Values are sent between devices in bfloat16 or wider.
A program may use at most 768 MiB of HBM per device.

```python
import jax
import jax.numpy as jnp
from jax import lax

S = 8192
D = 4096
HEADS = 32
HEAD = 128


def setup_inputs(seed: int = 0, part: int = 0) -> dict:
    k_shared, k_part = jax.random.split(jax.random.PRNGKey(seed))
    kx, kf, ku = jax.random.split(jax.random.fold_in(k_part, part), 3)
    kg, kq, ko = jax.random.split(k_shared, 3)
    r = jnp.arange(S, dtype=jnp.float32)[:, None] / S
    freq = jnp.array([0.5, 1.0, 1.5, 2.5], jnp.float32)
    phase = jax.random.uniform(kf, (4,), jnp.float32, 0.0, 2.0 * jnp.pi)
    waves = jnp.sin(2.0 * jnp.pi * r * freq + phase)
    u = jax.random.normal(ku, (4, D), jnp.float32)
    x = 0.25 * jax.random.normal(kx, (S, D), jnp.float32) + 0.35 * (waves @ u)
    g = 1.0 + 0.2 * jax.random.normal(kg, (D,), jnp.float32)
    wqkv = jax.random.normal(kq, (D, 3, HEADS, HEAD), jnp.float32) * D ** -0.5
    wo = jax.random.normal(ko, (HEADS, HEAD, D), jnp.float32) * (HEADS * HEAD) ** -0.5
    return {"x": x.astype(jnp.bfloat16), "g": g, "wqkv": wqkv.astype(jnp.bfloat16), "wo": wo.astype(jnp.bfloat16)}


def _rope(x, pos):
    half = HEAD // 2
    inv = 10000.0 ** (-jnp.arange(half, dtype=jnp.float32) * 2.0 / HEAD)
    ang = pos[:, None] * inv[None, :]
    cos = jnp.cos(ang)[:, None, :]
    sin = jnp.sin(ang)[:, None, :]
    x1, x2 = x[..., :half], x[..., half:]
    return jnp.concatenate([x1 * cos - x2 * sin, x2 * cos + x1 * sin], axis=-1)


def reference(x, g, wqkv, wo):
    xf = x.astype(jnp.float32)
    xn = (xf * lax.rsqrt(jnp.mean(xf * xf, axis=-1, keepdims=True) + 1e-5) * g).astype(jnp.bfloat16)
    qkv = jnp.dot(xn, wqkv.reshape(D, 3 * HEADS * HEAD), preferred_element_type=jnp.float32).reshape(S, 3, HEADS, HEAD)
    pos = jnp.arange(S, dtype=jnp.float32)
    q = _rope(qkv[:, 0], pos).astype(jnp.bfloat16)
    k = _rope(qkv[:, 1], pos).astype(jnp.bfloat16)
    v = qkv[:, 2].astype(jnp.bfloat16)
    qb = min(S, 512)
    nq = S // qb
    scale = HEAD ** -0.5

    def one_head(args):
        qh, kh, vh = args

        def one_block(a):
            qblk, i = a
            sc = jnp.dot(qblk, kh.T, preferred_element_type=jnp.float32) * scale
            mask = (i * qb + jnp.arange(qb))[:, None] >= jnp.arange(S)[None, :]
            sc = jnp.where(mask, sc, -jnp.inf)
            pr = jax.nn.softmax(sc, axis=-1).astype(jnp.bfloat16)
            return jnp.dot(pr, vh, preferred_element_type=jnp.float32).astype(jnp.bfloat16)

        o = lax.map(one_block, (qh.reshape(nq, qb, HEAD), jnp.arange(nq)))
        return o.reshape(S, HEAD)

    o = lax.map(one_head, (q.transpose(1, 0, 2), k.transpose(1, 0, 2), v.transpose(1, 0, 2)))
    o = o.transpose(1, 0, 2).reshape(S, HEADS * HEAD)
    y = xf + jnp.dot(o, wo.reshape(HEADS * HEAD, D), preferred_element_type=jnp.float32)
    return y.astype(jnp.bfloat16)
```

```python
import functools
import math

import jax
import jax.numpy as jnp
from jax import lax
from jax.experimental import pallas as pl
from jax.experimental.pallas import tpu as pltpu
from jax.sharding import PartitionSpec as P

BF = jnp.bfloat16
F32 = jnp.float32
MESH = pl.DeviceIdType.MESH


def _place(n):
    me = lax.axis_index("seq")
    core = lax.rem(me, 2)
    x = lax.rem(me // 2, n)
    y = me // (2 * n)
    return y, x, core, (lambda yy, xx, cc: {"seq": (yy * n + xx) * 2 + cc})


def _qkv_kernel(n, nc, ahead, x_ref, g_ref, cos_ref, sin_ref, w_ref, out_ref,
                xg, wst, wf, w, yst, rb, wsem, xs_s, xs_r, rl_s, ys_s, ys_r, rb_s, rb_r, fw_s, loc_s):
    t, d = x_ref.shape
    r = t // nc
    dk = wst.shape[1]
    y, x, core, dev = _place(n)
    step_x = 1 - 2 * core
    xf_, xb_ = lax.rem(x + step_x + n, n), lax.rem(x - step_x + n, n)
    yf_, yb_ = lax.rem(y + step_x + n, n), lax.rem(y - step_x + n, n)
    xo = lax.rem(x + 2, n)
    xslot = (x, xb_, xf_, xo)
    yd = [lax.rem(y + k, n) for k in range(n)]

    barrier = pltpu.get_barrier_semaphore()
    peers = [dev(y, xf_, core), dev(y, xb_, core), dev(y, x, 1 - core)]
    peers += [dev(yd[k], x, cc) for k in (1, n - 1) for cc in (0, 1)]
    for p_ in peers:
        pl.semaphore_signal(barrier, inc=1, device_id=p_, device_id_type=MESH)

    hb = x * (2 * n)

    def wload(i):
        return pltpu.make_async_copy(
            w_ref.at[pl.ds(pl.multiple_of(i * dk, dk), dk), :, pl.ds(pl.multiple_of(hb, 2 * n), 2 * n), :],
            wst.at[lax.rem(i, 2)], wsem.at[lax.rem(i, 2)])

    wload(0).start()
    wload(1).start()

    def norm(j, _):
        xv = x_ref[pl.ds(pl.multiple_of(j * r, r), r), :].astype(F32)
        v = xv * lax.rsqrt(jnp.mean(xv * xv, axis=-1, keepdims=True) + 1e-5) * g_ref[...]
        xg[j, 0] = v.astype(BF)
        return 0

    lax.fori_loop(0, nc, norm, 0)
    pl.semaphore_wait(barrier, len(peers))

    def own(j, k):
        return pltpu.make_async_remote_copy(
            xg.at[j, 0], xg.at[j, 1 + k], xs_s.at[k, j], xs_r.at[k, j],
            device_id=dev(y, (xf_, xb_)[k], core), device_id_type=MESH)

    def relay(j):
        return pltpu.make_async_remote_copy(
            xg.at[j, 1], xg.at[j, 3], rl_s.at[j], xs_r.at[2, j],
            device_id=dev(y, xf_, core), device_id_type=MESH)

    for j in range(ahead):
        own(j, 0).start()
        own(j, 1).start()

    nw = d // dk
    sub = wf.shape[1] // (2 * n)

    def relayout(i, _):
        wload(i).wait()
        slot = lax.rem(i, 2)
        for s in range(dk // sub):
            for c in range(3):
                b = (s * 3 + c) % 2
                wf[b] = wst[slot, s * sub:(s + 1) * sub, c, :, :].astype(F32).reshape(sub * 2 * n, 128)
                for h in range(2 * n):
                    rows = wf[b, pl.ds(h, sub, stride=2 * n), :]
                    w[h // 2, pl.ds(pl.multiple_of(i * dk + s * sub, sub), sub),
                      ((h % 2) * 3 + c) * 128:((h % 2) * 3 + c + 1) * 128] = rows.astype(BF)

        @pl.when(i + 2 < nw)
        def _():
            wload(i + 2).start()

        @pl.when(i == nw // 2)
        def _():
            own(0, 0).wait_recv()
            relay(0).start()
        return 0

    lax.fori_loop(0, nw, relayout, 0)

    def near(j, k, cc):
        return pltpu.make_async_remote_copy(
            yst.at[j, k, cc], out_ref.at[:, y, :, core, j], ys_s.at[k, cc, j], ys_r.at[k, core, j],
            device_id=dev(yd[k], x, cc), device_id_type=MESH)

    def sibling(j):
        return pltpu.make_async_remote_copy(
            yst.at[j, 0, 1 - core], out_ref.at[:, y, :, core, j], ys_s.at[0, 1, j], ys_r.at[0, core, j],
            device_id=dev(y, x, 1 - core), device_id_type=MESH)

    def local(j):
        return pltpu.make_async_copy(yst.at[j, 0, core], out_ref.at[:, y, :, core, j], loc_s.at[j])

    def hop(j):
        return pltpu.make_async_remote_copy(
            yst.at[j, 2], rb.at[j], rb_s.at[j], rb_r.at[j],
            device_id=dev(yf_, x, core), device_id_type=MESH)

    def forward(j, cc):
        return pltpu.make_async_remote_copy(
            rb.at[j, cc], out_ref.at[:, yb_, :, core, j], fw_s.at[cc, j], ys_r.at[2, core, j],
            device_id=dev(yf_, x, cc), device_id_type=MESH)

    def step(j, _):
        @pl.when(j + ahead < nc)
        def _():
            own(j + ahead, 0).start()
            own(j + ahead, 1).start()

        @pl.when(j + 1 < nc)
        def _():
            own(j + 1, 0).wait_recv()
            relay(j + 1).start()

        @pl.when(j >= 1)
        def _():
            hop(j - 1).wait_recv()
            forward(j - 1, 0).start()
            forward(j - 1, 1).start()

        own(j, 1).wait_recv()
        relay(j).wait_recv()
        lhs = xg[j].reshape(4 * r, d)
        cosv = jnp.concatenate([cos_ref[xs, j] for xs in xslot], axis=0)
        sinv = jnp.concatenate([sin_ref[xs, j] for xs in xslot], axis=0)
        for k in (2, 1, 3, 0):
            acc = jnp.dot(lhs, w[yd[k]], preferred_element_type=F32)
            for cc in range(2):
                for c in range(3):
                    v = acc[:, (cc * 3 + c) * 128:(cc * 3 + c + 1) * 128]
                    if c < 2:
                        v = v * cosv + pltpu.roll(v, 64, 1) * sinv
                    v = v.astype(BF)
                    for s in range(4):
                        yst[j, k, cc, c, xslot[s]] = v[s * r:(s + 1) * r]
            if k == 2:
                hop(j).start()
            elif k == 0:
                sibling(j).start()
                local(j).start()
            else:
                near(j, k, 0).start()
                near(j, k, 1).start()
        return 0

    lax.fori_loop(0, nc, step, 0)
    hop(nc - 1).wait_recv()
    forward(nc - 1, 0).start()
    forward(nc - 1, 1).start()

    def drain(j, _):
        for k in range(2):
            own(j, k).wait_send()
        relay(j).wait_send()
        hop(j).wait_send()
        for cc in range(2):
            forward(j, cc).wait_send()
            for k in (1, 3):
                near(j, k, cc).wait_send()
        sibling(j).wait_send()
        local(j).wait()
        for k in (1, 2, 3):
            for cc in range(2):
                pltpu.make_async_remote_copy(
                    yst.at[j, k, cc], out_ref.at[:, yd[n - k], :, cc, j], ys_s.at[k, cc, j], ys_r.at[k, cc, j],
                    device_id=dev(y, x, 1 - core), device_id_type=MESH).wait_recv()
        pltpu.make_async_remote_copy(
            yst.at[j, 0, core], out_ref.at[:, y, :, 1 - core, j], ys_s.at[0, 1, j], ys_r.at[0, 1 - core, j],
            device_id=dev(y, x, 1 - core), device_id_type=MESH).wait_recv()
        return 0

    lax.fori_loop(0, nc, drain, 0)


def qkv_exchange(n, nc, ahead, x, g, cos, sin, wqkv):
    t, d = x.shape
    h, dh = wqkv.shape[2:]
    r = t // nc
    dk = 128
    vm = pl.BlockSpec(memory_space=pltpu.VMEM)
    dma = pltpu.SemaphoreType.DMA
    return pl.pallas_call(
        functools.partial(_qkv_kernel, n, nc, ahead),
        out_shape=jax.ShapeDtypeStruct((3, n, n, 2, nc, r, dh), BF),
        in_specs=[vm, vm, vm, vm, pl.BlockSpec(memory_space=pl.ANY)],
        out_specs=pl.BlockSpec(memory_space=pl.ANY),
        scratch_shapes=[
            pltpu.VMEM((nc, 4, r, d), BF),
            pltpu.VMEM((2, dk, 3, 2 * n, dh), BF),
            pltpu.VMEM((2, 32 * 2 * n, dh), F32),
            pltpu.VMEM((n, d, 6 * dh), BF),
            pltpu.VMEM((nc, n, 2, 3, n, r, dh), BF),
            pltpu.VMEM((nc, 2, 3, n, r, dh), BF),
            dma((2,)), dma((2, nc)), dma((3, nc)), dma((nc,)),
            dma((n, 2, nc)), dma((n, 2, nc)), dma((nc,)), dma((nc,)), dma((2, nc)), dma((nc,)),
        ],
        compiler_params=pltpu.CompilerParams(collective_id=0, has_side_effects=True, vmem_limit_bytes=64 * 2**20 - 2**16),
        cost_estimate=pl.CostEstimate(flops=2 * t * d * 3 * h * dh, bytes_accessed=40 * 2**20, transcendentals=0),
    )(x, g.reshape(1, d), cos, sin, wqkv)


def tables(n, t, dh, nc):
    y, x, core, _ = _place(n)
    pos = (((y * n + jnp.arange(n))[:, None] * 2 + core) * t + jnp.arange(t)[None, :]).astype(F32)
    inv = 10000.0 ** (-jnp.arange(dh // 2, dtype=F32) * 2.0 / dh)
    ang = pos[..., None] * inv
    cos, sin = jnp.cos(ang), jnp.sin(ang)
    shape = (n, nc, t // nc, dh)
    return jnp.concatenate([cos, cos], -1).reshape(shape), jnp.concatenate([-sin, sin], -1).reshape(shape)


NEG = -1e30

def flash_kernel(q_ref, k_ref, v_ref, o_ref, vt_ref, qt_ref, s_ref, acc_ref, m_ref, l_ref, *, bq, bk, qt, sub, mxl, pre):
    i = pl.program_id(0)
    S, d = k_ref.shape
    c = (d ** -0.5) * math.log2(math.e)
    dv = vt_ref.shape[0]

    @pl.when(i == 0)
    def _():
        if mxl:
            vt_ref[d:, :] = jnp.ones((dv - d, S), jnp.bfloat16)
        def tr(j, _):
            blk = pl.ds(pl.multiple_of(j * 512, 512), 512)
            vt_ref[0:d, blk] = v_ref[blk, :].T
            return 0
        lax.fori_loop(0, S // 512, tr, 0)
    if pre:
        qt_ref[...] = q_ref[...].T
    acc_ref[...] = jnp.zeros_like(acc_ref)
    m_ref[...] = jnp.full_like(m_ref, NEG)
    l_ref[...] = jnp.zeros_like(l_ref)

    def block(k0, n, masked):
        for t in range(bq // qt):
            cols = slice(t * qt, (t + 1) * qt)
            if masked:
                nn = min(n, (t + 1) * qt)
            else:
                nn = n
            m_old = m_ref[:, cols]
            m_new = m_old
            ss = []
            step = min(nn, 512)
            for u in range(nn // step):
                ks = pl.ds(pl.multiple_of(k0 + u * step, step), step)
                if pre:
                    s = jnp.dot(k_ref[ks, :], qt_ref[:, cols], preferred_element_type=jnp.float32)
                else:
                    s = lax.dot_general(k_ref[ks, :], q_ref[cols, :], (((1,), (1,)), ((), ())), preferred_element_type=jnp.float32)
                if masked:
                    kp = lax.broadcasted_iota(jnp.int32, s.shape, 0) + u * step
                    qp = lax.broadcasted_iota(jnp.int32, s.shape, 1) + t * qt
                    s = jnp.where(kp <= qp, s, NEG)
                s_ref[t % 2, u * step:(u + 1) * step, :] = s
                m_new = jnp.maximum(m_new, jnp.max(s, axis=0, keepdims=True))
            a = jnp.exp2((m_old - m_new) * c)
            mc = m_new * c
            l = l_ref[:, cols] * a
            acc = acc_ref[:, cols] * a
            part = None
            for u in range(nn // sub):
                ks = pl.ds(pl.multiple_of(k0 + u * sub, sub), sub)
                p = jnp.exp2(s_ref[t % 2, u * sub:(u + 1) * sub, :] * c - mc)
                if not mxl:
                    l = l + jnp.sum(p, axis=0, keepdims=True)
                dd = jnp.dot(vt_ref[:, ks], p.astype(jnp.bfloat16), preferred_element_type=jnp.float32)
                part = dd if part is None else part + dd
            m_ref[:, cols] = m_new
            l_ref[:, cols] = l
            acc_ref[:, cols] = acc + part

    nfull = (i * bq) // bk
    lax.fori_loop(0, nfull, lambda j, _: (block(j * bk, bk, False), 0)[1], 0)
    rest0 = nfull * bk
    if bk > bq:
        nrest = (i * bq - rest0) // bq
        lax.fori_loop(0, nrest, lambda j, _: (block(rest0 + j * bq, bq, False), 0)[1], 0)
    block(i * bq, bq, True)
    l = acc_ref[d:d + 1, :] if mxl else l_ref[...]
    o = acc_ref[0:d, :] * (1.0 / l)
    o_ref[...] = o.T.astype(o_ref.dtype)

def flash(q, k, v, bq=512, bk=2048, qt=512, sub=256, mxl=0, pre=1):
    S, d = q.shape
    dv = d + 16 * mxl
    whole = pl.BlockSpec((S, d), lambda i: (0, 0))
    return pl.pallas_call(
        functools.partial(flash_kernel, bq=bq, bk=bk, qt=qt, sub=sub, mxl=mxl, pre=pre),
        out_shape=jax.ShapeDtypeStruct((S, d), jnp.bfloat16),
        grid=(S // bq,),
        in_specs=[pl.BlockSpec((bq, d), lambda i: (i, 0)), whole, whole],
        out_specs=pl.BlockSpec((bq, d), lambda i: (i, 0)),
        scratch_shapes=[pltpu.VMEM((dv, S), jnp.bfloat16), pltpu.VMEM((d, bq), jnp.bfloat16), pltpu.VMEM((2, max(bk, bq), qt), jnp.float32), pltpu.VMEM((dv, bq), jnp.float32),
                        pltpu.VMEM((1, bq), jnp.float32), pltpu.VMEM((1, bq), jnp.float32)],
        compiler_params=pltpu.CompilerParams(dimension_semantics=("arbitrary",), vmem_limit_bytes=60 * 2**20),
    )(q, k, v)


def solution(mesh):
    p = mesh.shape["seq"]
    n = math.isqrt(p // 2)
    rows = P(("data", "seq"), None)
    chunks, ahead = 8, 3

    def local(x, g, wqkv, wo):
        t, d = x.shape
        h, dh = wqkv.shape[2:]
        cos, sin = tables(n, t, dh, chunks)
        qkv = qkv_exchange(n, chunks, ahead, x, g, cos, sin, wqkv).reshape(3, p * t, dh)
        o = flash(qkv[0], qkv[1], qkv[2], 2048, 2048, 512, 256, 1, 1)
        o = lax.all_to_all(o.reshape(p, t, dh), "seq", 0, 0, tiled=True)
        o = o.reshape(n, n, 2, t, dh).transpose(3, 1, 0, 2, 4).reshape(t, h * dh)
        y = x.astype(F32) + jnp.dot(o, wo.reshape(h * dh, d), preferred_element_type=F32)
        return y.astype(x.dtype)

    return jax.shard_map(local, mesh=mesh,
                         in_specs=(rows, P(None), P(None, None, None, None), P(None, None, None)),
                         out_specs=rows, check_vma=False)
```

```python
import functools
import math

import jax
import jax.numpy as jnp
from jax import lax
from jax.experimental import pallas as pl
from jax.experimental.pallas import tpu as pltpu
from jax.sharding import PartitionSpec as P

BF = jnp.bfloat16
F32 = jnp.float32
MESH = pl.DeviceIdType.MESH


def _place(n):
    me = lax.axis_index("seq")
    core = lax.rem(me, 2)
    x = lax.rem(me // 2, n)
    y = me // (2 * n)
    return y, x, core, (lambda yy, xx, cc: {"seq": (yy * n + xx) * 2 + cc})


def _qkv_kernel(n, nc, ahead, x_ref, g_ref, cos_ref, sin_ref, w_ref, out_ref,
                xo, xg, wst, w, yo, yst, ro, rb, wsem, xs_s, xs_r, rl_s, ys_s, ys_r, rb_s, rb_r, fw_s, loc_s):
    t, d = x_ref.shape
    r = t // nc
    dk = wst.shape[1]
    y, x, core, dev = _place(n)
    way = 1 - 2 * core
    xf_, xb_ = lax.rem(x + way + n, n), lax.rem(x - way + n, n)
    yf_, yb_ = lax.rem(y + way + n, n), lax.rem(y - way + n, n)
    xslot = (xb_, xf_, lax.rem(x + 2, n))
    yd = [lax.rem(y + k, n) for k in range(n)]

    barrier = pltpu.get_barrier_semaphore()
    peers = [dev(y, xf_, core), dev(y, xb_, core), dev(y, x, 1 - core)]
    peers += [dev(yd[k], x, cc) for k in (1, n - 1) for cc in (0, 1)]
    for p_ in peers:
        pl.semaphore_signal(barrier, inc=1, device_id=p_, device_id_type=MESH)

    hb = x * (2 * n)
    nw = d // dk
    nb = wst.shape[0]

    def wload(i):
        return pltpu.make_async_copy(
            w_ref.at[pl.ds(pl.multiple_of(i * dk, dk), dk), :, pl.ds(pl.multiple_of(hb, 2 * n), 2 * n), :],
            wst.at[lax.rem(i, nb)], wsem.at[lax.rem(i, nb)])

    for i in range(nb):
        wload(i).start()

    def rows_of(j):
        return pl.ds(pl.multiple_of(j * r, r), r)

    def norm(j, _):
        xv = x_ref[rows_of(j), :].astype(F32)
        v = xv * lax.rsqrt(jnp.mean(xv * xv, axis=-1, keepdims=True) + 1e-5) * g_ref[...]
        xo[rows_of(j), :] = v.astype(BF)
        return 0

    def own(j, k):
        return pltpu.make_async_remote_copy(
            xo.at[rows_of(j), :], xg.at[j, k], xs_s.at[k, j], xs_r.at[k, j],
            device_id=dev(y, (xf_, xb_)[k], core), device_id_type=MESH)

    def relay(j):
        return pltpu.make_async_remote_copy(
            xg.at[j, 0], xg.at[j, 2], rl_s.at[j], xs_r.at[2, j],
            device_id=dev(y, xf_, core), device_id_type=MESH)

    lax.fori_loop(0, ahead, norm, 0)
    pl.semaphore_wait(barrier, len(peers))
    for j in range(ahead):
        own(j, 0).start()
        own(j, 1).start()
    lax.fori_loop(ahead, nc, norm, 0)
    sub = 32

    def relayout(i, _):
        wload(i).wait()
        slot = lax.rem(i, nb)
        for s in range(dk // sub):
            for c in range(3):
                vv = jnp.swapaxes(wst[slot, s * sub:(s + 1) * sub, c, :, :], 0, 1)
                for h in range(2 * n):
                    w[h // 2, pl.ds(pl.multiple_of(i * dk + s * sub, sub), sub),
                      ((h % 2) * 3 + c) * 128:((h % 2) * 3 + c + 1) * 128] = vv[h]

        @pl.when(i + nb < nw)
        def _():
            wload(i + nb).start()
        return 0

    lax.fori_loop(0, nw, relayout, 0)
    own(0, 0).wait_recv()
    relay(0).start()

    def at(whole, parts, j):
        return whole if j is None else parts.at[j]

    def sj(j):
        return nc if j is None else j

    def dst(yy, cc, j):
        return out_ref.at[:, yy, 0, cc] if j is None else out_ref.at[:, yy, pl.ds(1, 3), cc, rows_of(j)]

    def near(j, k, cc):
        return pltpu.make_async_remote_copy(
            at(yo, yst, j).at[k, cc], dst(y, core, j), ys_s.at[k, cc, sj(j)], ys_r.at[k, core, sj(j)],
            device_id=dev(yd[k], x, cc), device_id_type=MESH)

    def sibling(j):
        return pltpu.make_async_remote_copy(
            at(yo, yst, j).at[0, 1 - core], dst(y, core, j), ys_s.at[0, 1, sj(j)], ys_r.at[0, core, sj(j)],
            device_id=dev(y, x, 1 - core), device_id_type=MESH)

    def local(j):
        return pltpu.make_async_copy(at(yo, yst, j).at[0, core], dst(y, core, j), loc_s.at[sj(j)])

    def hop(j):
        return pltpu.make_async_remote_copy(
            at(yo, yst, j).at[2], at(ro, rb, j), rb_s.at[sj(j)], rb_r.at[sj(j)],
            device_id=dev(yf_, x, core), device_id_type=MESH)

    def forward(j, cc):
        return pltpu.make_async_remote_copy(
            at(ro, rb, j).at[cc], dst(yb_, core, j), fw_s.at[cc, sj(j)], ys_r.at[2, core, sj(j)],
            device_id=dev(yf_, x, cc), device_id_type=MESH)

    def pass_on(j):
        hop(j).wait_recv()
        forward(j, 0).start()
        forward(j, 1).start()

    def project(j, lhs, cosv, sinv, after_hop):
        for k in (2, 1, 3, 0):
            acc = jnp.dot(lhs, w[yd[k]], preferred_element_type=F32)
            for cc in range(2):
                for c in range(3):
                    v = acc[:, (cc * 3 + c) * 128:(cc * 3 + c + 1) * 128]
                    if c < 2:
                        v = v * cosv + pltpu.roll(v, 64, 1) * sinv
                    v = v.astype(BF)
                    if j is None:
                        yo[k, cc, c] = v
                    else:
                        yst[j, k, cc, c] = v.reshape(3, r, 128)
            if k == 2:
                hop(j).start()
                after_hop()
            elif k == 0:
                sibling(j).start()
                local(j).start()
            else:
                near(j, k, 0).start()
                near(j, k, 1).start()

    project(None, xo[...], cos_ref[x].reshape(t, 128), sin_ref[x].reshape(t, 128), lambda: None)

    def step(j, _):
        @pl.when(j + ahead < nc)
        def _():
            own(j + ahead, 0).start()
            own(j + ahead, 1).start()

        @pl.when(j + 1 < nc)
        def _():
            own(j + 1, 0).wait_recv()
            relay(j + 1).start()

        own(j, 1).wait_recv()
        relay(j).wait_recv()
        lhs = xg[j].reshape(3 * r, d)
        cosv = jnp.concatenate([cos_ref[xs, j] for xs in xslot], axis=0)
        sinv = jnp.concatenate([sin_ref[xs, j] for xs in xslot], axis=0)

        def after_hop():
            @pl.when(j == 0)
            def _():
                pass_on(None)

            @pl.when(j > 0)
            def _():
                pass_on(j - 1)

        project(j, lhs, cosv, sinv, after_hop)
        return 0

    lax.fori_loop(0, nc, step, 0)
    pass_on(nc - 1)

    def finish(j):
        hop(j).wait_send()
        for cc in range(2):
            forward(j, cc).wait_send()
            for k in (1, 3):
                near(j, k, cc).wait_send()
        sibling(j).wait_send()
        local(j).wait()
        for k in (1, 2, 3):
            for cc in range(2):
                pltpu.make_async_remote_copy(
                    at(yo, yst, j).at[k, cc], dst(yd[n - k], cc, j), ys_s.at[k, cc, sj(j)], ys_r.at[k, cc, sj(j)],
                    device_id=dev(y, x, 1 - core), device_id_type=MESH).wait_recv()
        pltpu.make_async_remote_copy(
            at(yo, yst, j).at[0, core], dst(y, 1 - core, j), ys_s.at[0, 1, sj(j)], ys_r.at[0, 1 - core, sj(j)],
            device_id=dev(y, x, 1 - core), device_id_type=MESH).wait_recv()

    finish(None)

    def drain(j, _):
        for k in range(2):
            own(j, k).wait_send()
        relay(j).wait_send()
        finish(j)
        return 0

    lax.fori_loop(0, nc, drain, 0)


def qkv_exchange(n, nc, ahead, x, g, cos, sin, wqkv):
    t, d = x.shape
    h, dh = wqkv.shape[2:]
    r = t // nc
    dk = 128
    vm = pl.BlockSpec(memory_space=pltpu.VMEM)
    dma = pltpu.SemaphoreType.DMA
    return pl.pallas_call(
        functools.partial(_qkv_kernel, n, nc, ahead),
        out_shape=jax.ShapeDtypeStruct((3, n, 4, 2, t, dh), BF),
        in_specs=[vm, vm, vm, vm, pl.BlockSpec(memory_space=pl.ANY)],
        out_specs=pl.BlockSpec(memory_space=pl.ANY),
        scratch_shapes=[
            pltpu.VMEM((t, d), BF),
            pltpu.VMEM((nc, 3, r, d), BF),
            pltpu.VMEM((6, dk, 3, 2 * n, dh), BF),
            pltpu.VMEM((n, d, 6 * dh), BF),
            pltpu.VMEM((n, 2, 3, t, dh), BF),
            pltpu.VMEM((nc, n, 2, 3, 3, r, dh), BF),
            pltpu.VMEM((2, 3, t, dh), BF),
            pltpu.VMEM((nc, 2, 3, 3, r, dh), BF),
            dma((6,)), dma((2, nc)), dma((3, nc)), dma((nc,)),
            dma((n, 2, nc + 1)), dma((n, 2, nc + 1)), dma((nc + 1,)), dma((nc + 1,)), dma((2, nc + 1)), dma((nc + 1,)),
        ],
        compiler_params=pltpu.CompilerParams(collective_id=0, has_side_effects=True, vmem_limit_bytes=64 * 2**20 - 2**16),
        cost_estimate=pl.CostEstimate(flops=2 * t * d * 3 * h * dh, bytes_accessed=40 * 2**20, transcendentals=0),
    )(x, g.reshape(1, d), cos, sin, wqkv)


def tables(n, t, dh, nc):
    y, x, core, _ = _place(n)
    pos = (((y * n + jnp.arange(n))[:, None] * 2 + core) * t + jnp.arange(t)[None, :]).astype(F32)
    inv = 10000.0 ** (-jnp.arange(dh // 2, dtype=F32) * 2.0 / dh)
    ang = pos[..., None] * inv
    cos, sin = jnp.cos(ang), jnp.sin(ang)
    shape = (n, nc, t // nc, dh)
    return jnp.concatenate([cos, cos], -1).reshape(shape), jnp.concatenate([-sin, sin], -1).reshape(shape)


NEG = -1e30


def _attn_kernel(n, qt, bk, sub, qkv_ref, x_ref, wo_ref, y_ref,
                 qkv, xv, wo, ob, acc, yacc, vt, qtr, sa, sb, m, ma, mb, insem, wosem, osem, rsem):
    q, k, v = qkv.at[0], qkv.at[1], qkv.at[2]
    s_len, d = k.shape
    t = ob.shape[0]
    dv = vt.shape[0]
    p = s_len // t
    groups = s_len // qt
    per = qt // t
    c = (d ** -0.5) * math.log2(math.e)
    me = lax.axis_index("seq")
    y, x, core, _ = _place(n)
    head = (x * n + y) * 2 + core
    rot = head // (p // groups)
    my_tile = me // per

    def dev_head(h):
        return (lax.rem(h // 2, n) * n + h // (2 * n)) * 2 + lax.rem(h, 2)

    barrier = pltpu.get_barrier_semaphore()

    def greet(i, _):
        pl.semaphore_signal(barrier, inc=1, device_id={"seq": lax.rem(me + i, p)}, device_id_type=MESH)
        return 0

    lax.fori_loop(1, p, greet, 0)
    for yy in range(n):
        for slot in range(4):
            for cc in range(2):
                off = (0, 2 * cc - 1, 1 - 2 * cc, 2)[slot]
                row = ((yy * n + lax.rem(x + off + n, n)) * 2 + cc) * t
                pltpu.make_async_copy(qkv_ref.at[:, yy, slot, cc], qkv.at[:, pl.ds(pl.multiple_of(row, t), t), :],
                                      insem.at[0]).start()
    pltpu.make_async_copy(x_ref, xv, insem.at[1]).start()
    kw = wo.shape[0] // groups

    def wload(g):
        rows = pl.ds(pl.multiple_of(g * kw, kw), kw)
        return pltpu.make_async_copy(wo_ref.at[rows, :], wo.at[rows, :], wosem.at[g])

    for g in range(groups):
        wload(g).start()
    vt[d:, :] = jnp.ones((dv - d, s_len), BF)
    pltpu.make_async_copy(qkv, qkv, insem.at[0]).wait()

    def tr(j, _):
        blk = pl.ds(pl.multiple_of(j * 512, 512), 512)
        vt[0:d, blk] = v[blk, :].T
        return 0

    lax.fori_loop(0, s_len // 512, tr, 0)

    def qk(j, s_ref, mm, bias=None):
        mx = None
        qv = qtr[...]
        for u in range(bk // sub):
            ks = pl.ds(pl.multiple_of(j * bk + u * sub, sub), sub)
            s = jnp.dot(k[ks, :], qv, preferred_element_type=F32)
            if bias is not None:
                kp = lax.broadcasted_iota(jnp.int32, s.shape, 0) + u * sub
                qp = lax.broadcasted_iota(jnp.int32, s.shape, 1)
                s = jnp.where(kp - qp <= bias, s, NEG)
            s_ref[u * sub:(u + 1) * sub, :] = s
            sm = jnp.max(s, axis=0, keepdims=True)
            mx = sm if mx is None else jnp.maximum(mx, sm)
        mm[...] = mx

    def pv(j, s_ref, mm):
        m_old = m[...]
        m_new = jnp.maximum(m_old, mm[...])
        a = jnp.exp2((m_old - m_new) * c)
        mc = m_new * c
        part = None
        for u in range(bk // sub):
            ks = pl.ds(pl.multiple_of(j * bk + u * sub, sub), sub)
            pr = jnp.exp2(s_ref[u * sub:(u + 1) * sub, :] * c - mc)
            dd = jnp.dot(vt[:, ks], pr.astype(BF), preferred_element_type=F32)
            part = dd if part is None else part + dd
        m[...] = m_new
        acc[...] = acc[...] * a + part

    def send(tile, e):
        to = tile * per + e
        return pltpu.make_async_remote_copy(
            v.at[pl.ds(pl.multiple_of(tile * qt + e * t, t), t), :], ob.at[:, pl.ds(pl.multiple_of(head * d, d), d)],
            osem.at[tile, e], rsem.at[head], device_id={"seq": to}, device_id_type=MESH)

    def keep(tile, e):
        return pltpu.make_async_copy(
            v.at[pl.ds(pl.multiple_of(tile * qt + e * t, t), t), :], ob.at[:, pl.ds(pl.multiple_of(head * d, d), d)], osem.at[tile, e])

    def tile_body(i, _):
        tile = lax.rem(i + rot, groups)
        rows = pl.ds(pl.multiple_of(tile * qt, qt), qt)
        qtr[...] = q[rows, :].T
        acc[...] = jnp.zeros_like(acc)
        m[...] = jnp.full_like(m, NEG)
        last = (tile * qt) // bk
        bias = tile * qt - last * bk

        @pl.when(last == 0)
        def _():
            qk(0, sa, ma, bias)
            pv(0, sa, ma)

        @pl.when(last > 0)
        def _():
            qk(0, sa, ma)

            def pair(jj, _):
                qk(2 * jj + 1, sb, mb)
                pv(2 * jj, sa, ma)
                qk(2 * jj + 2, sa, ma)
                pv(2 * jj + 1, sb, mb)
                return 0

            npair = (last - 1) // 2
            lax.fori_loop(0, npair, pair, 0)
            b0 = 2 * npair

            @pl.when(last - b0 == 1)
            def _():
                qk(last, sb, mb, bias)
                pv(b0, sa, ma)
                pv(last, sb, mb)

            @pl.when(last - b0 == 2)
            def _():
                qk(b0 + 1, sb, mb)
                pv(b0, sa, ma)
                qk(last, sa, ma, bias)
                pv(b0 + 1, sb, mb)
                pv(last, sa, ma)

        o = acc[0:d, :] * (1.0 / acc[d:d + 1, :])
        v[rows, :] = o.T.astype(BF)

        @pl.when(i == 0)
        def _():
            pl.semaphore_wait(barrier, p - 1)

        for e in range(per):
            @pl.when(tile * per + e == me)
            def _():
                keep(tile, e).start()

            @pl.when(tile * per + e != me)
            def _():
                send(tile, e).start()
        return 0

    lax.fori_loop(0, groups, tile_body, 0)
    pltpu.make_async_copy(x_ref, xv, insem.at[1]).wait()
    hp = p // groups
    cw = 1024

    def arrive(h):
        @pl.when(h == head)
        def _():
            keep(my_tile, lax.rem(me, per)).wait()

        @pl.when(h != head)
        def _():
            pltpu.make_async_remote_copy(
                v.at[pl.ds(0, t), :], ob.at[:, pl.ds(pl.multiple_of(h * d, d), d)],
                osem.at[0, 0], rsem.at[h], device_id={"seq": dev_head(h)}, device_id_type=MESH).wait_recv()

    def project(i, _):
        g = lax.rem(my_tile - i + groups, groups)
        wload(g).wait()
        for e in range(hp):
            arrive(g * hp + e)
        o = ob[:, pl.ds(pl.multiple_of(g * kw, kw), kw)]

        def cols(j, _):
            cs = pl.ds(pl.multiple_of(j * cw, cw), cw)
            dd = jnp.dot(o, wo[pl.ds(pl.multiple_of(g * kw, kw), kw), cs], preferred_element_type=F32)

            @pl.when(i == 0)
            def _():
                yacc[:, cs] = xv[:, cs].astype(F32) + dd

            @pl.when(jnp.logical_and(i > 0, i < groups - 1))
            def _():
                yacc[:, cs] = yacc[:, cs] + dd

            @pl.when(i == groups - 1)
            def _():
                y_ref[:, cs] = (yacc[:, cs] + dd).astype(BF)
            return 0

        lax.fori_loop(0, wo.shape[1] // cw, cols, 0)
        return 0

    lax.fori_loop(0, groups, project, 0)

    def drain(tile, _):
        for e in range(per):
            @pl.when(tile * per + e != me)
            def _():
                send(tile, e).wait_send()
        return 0

    lax.fori_loop(0, groups, drain, 0)


def attend(n, qt, bk, sub, qkv, x, wo):
    t, dm = x.shape
    hd = wo.shape[0]
    d = qkv.shape[-1]
    p = 2 * n * n
    s_len = p * t
    groups = s_len // qt
    any_ = pl.BlockSpec(memory_space=pl.ANY)
    dma = pltpu.SemaphoreType.DMA

    return pl.pallas_call(
        functools.partial(_attn_kernel, n, qt, bk, sub),
        out_shape=jax.ShapeDtypeStruct((t, dm), BF),
        in_specs=[any_, any_, any_],
        out_specs=pl.BlockSpec(memory_space=pltpu.VMEM),
        scratch_shapes=[
            pltpu.VMEM((3, s_len, d), BF),
            pltpu.VMEM((t, dm), BF), pltpu.VMEM((hd, dm), BF), pltpu.VMEM((t, hd), BF),
            pltpu.VMEM((d + 16, qt), F32), pltpu.VMEM((t, dm), F32),
            pltpu.VMEM((d + 16, s_len), BF), pltpu.VMEM((d, qt), BF),
            pltpu.VMEM((bk, qt), F32), pltpu.VMEM((bk, qt), F32),
            pltpu.VMEM((1, qt), F32), pltpu.VMEM((1, qt), F32), pltpu.VMEM((1, qt), F32),
            dma((4,)), dma((groups,)), dma((groups, qt // t)), dma((p,)),
        ],
        compiler_params=pltpu.CompilerParams(collective_id=1, has_side_effects=True, vmem_limit_bytes=64 * 2**20 - 2**16),
        cost_estimate=pl.CostEstimate(flops=2 * s_len * s_len * d + 2 * t * hd * dm, bytes_accessed=2 * hd * dm, transcendentals=s_len * s_len // 2),
    )(qkv, x, wo)


def solution(mesh):
    p = mesh.shape["seq"]
    n = math.isqrt(p // 2)
    rows = P(("data", "seq"), None)
    chunks, ahead = 8, 3

    def local(x, g, wqkv, wo):
        t, d = x.shape
        h, dh = wqkv.shape[2:]
        cos, sin = tables(n, t, dh, chunks)
        qkv = qkv_exchange(n, chunks, ahead, x, g, cos, sin, wqkv)
        return attend(n, 1024, 1024, 512, qkv, x, wo.reshape(h * dh, d))

    return jax.shard_map(local, mesh=mesh,
                         in_specs=(rows, P(None), P(None, None, None, None), P(None, None, None)),
                         out_specs=rows, check_vma=False)
```

```python
import functools
import math

import jax
import jax.numpy as jnp
from jax import lax
from jax.experimental import pallas as pl
from jax.experimental.pallas import tpu as pltpu
from jax.sharding import PartitionSpec as P

BF = jnp.bfloat16
F32 = jnp.float32
MESH = pl.DeviceIdType.MESH


def _place(n):
    me = lax.axis_index("seq")
    core = lax.rem(me, 2)
    x = lax.rem(me // 2, n)
    y = me // (2 * n)
    return y, x, core, (lambda yy, xx, cc: {"seq": (yy * n + xx) * 2 + cc})


def _qkv_kernel(n, nc, ahead, x_ref, g_ref, inv_ref, w_ref, out_ref,
                xo, xg, wst, w, yo, yst, ro, rb, wsem, xs_s, xs_r, rl_s, ys_s, ys_r, rb_s, rb_r, fw_s, loc_s):
    t, d = x_ref.shape
    r = t // nc
    dk = wst.shape[1]
    y, x, core, dev = _place(n)
    way = 1 - 2 * core
    xf_, xb_ = lax.rem(x + way + n, n), lax.rem(x - way + n, n)
    yf_, yb_ = lax.rem(y + way + n, n), lax.rem(y - way + n, n)
    xslot = (xb_, xf_, lax.rem(x + 2, n))
    yd = [lax.rem(y + k, n) for k in range(n)]

    barrier = pltpu.get_barrier_semaphore()
    peers = [dev(y, xf_, core), dev(y, xb_, core), dev(y, x, 1 - core)]
    peers += [dev(yd[k], x, cc) for k in (1, n - 1) for cc in (0, 1)]
    for p_ in peers:
        pl.semaphore_signal(barrier, inc=1, device_id=p_, device_id_type=MESH)

    hb = x * (2 * n)
    nw = d // dk
    nb = wst.shape[0]

    def wload(i):
        return pltpu.make_async_copy(
            w_ref.at[pl.ds(pl.multiple_of(i * dk, dk), dk), :, pl.ds(pl.multiple_of(hb, 2 * n), 2 * n), :],
            wst.at[lax.rem(i, nb)], wsem.at[lax.rem(i, nb)])

    for i in range(nb):
        wload(i).start()

    def rows_of(j):
        return pl.ds(pl.multiple_of(j * r, r), r)

    def turn(xs, first, rows):
        pos = lax.broadcasted_iota(jnp.int32, (rows, 128), 0) + (((y * n + xs) * 2 + core) * t + first)
        ang = pos.astype(F32) * inv_ref[...]
        low = lax.broadcasted_iota(jnp.int32, (rows, 128), 1) < 64
        s = jnp.sin(ang)
        return jnp.cos(ang), jnp.where(low, -s, s)

    def norm(j, _):
        xv = x_ref[rows_of(j), :].astype(F32)
        v = xv * lax.rsqrt(jnp.mean(xv * xv, axis=-1, keepdims=True) + 1e-5) * g_ref[...]
        xo[rows_of(j), :] = v.astype(BF)
        return 0

    def own(j, k):
        return pltpu.make_async_remote_copy(
            xo.at[rows_of(j), :], xg.at[j, k], xs_s.at[k, j], xs_r.at[k, j],
            device_id=dev(y, (xf_, xb_)[k], core), device_id_type=MESH)

    def relay(j):
        return pltpu.make_async_remote_copy(
            xg.at[j, 0], xg.at[j, 2], rl_s.at[j], xs_r.at[2, j],
            device_id=dev(y, xf_, core), device_id_type=MESH)

    lax.fori_loop(0, ahead, norm, 0)
    pl.semaphore_wait(barrier, len(peers))
    for j in range(ahead):
        own(j, 0).start()
        own(j, 1).start()
    lax.fori_loop(ahead, nc, norm, 0)
    sub = 32

    def relayout(i, _):
        wload(i).wait()
        slot = lax.rem(i, nb)
        for s in range(dk // sub):
            for c in range(3):
                vv = jnp.swapaxes(wst[slot, s * sub:(s + 1) * sub, c, :, :], 0, 1)
                for h in range(2 * n):
                    w[h // 2, pl.ds(pl.multiple_of(i * dk + s * sub, sub), sub),
                      ((h % 2) * 3 + c) * 128:((h % 2) * 3 + c + 1) * 128] = vv[h]

        @pl.when(i + nb < nw)
        def _():
            wload(i + nb).start()
        return 0

    lax.fori_loop(0, nw, relayout, 0)
    own(0, 0).wait_recv()
    relay(0).start()

    def at(whole, parts, j):
        return whole if j is None else parts.at[j]

    def sj(j):
        return nc if j is None else j

    def dst(yy, cc, j):
        return out_ref.at[:, yy, 0, cc] if j is None else out_ref.at[:, yy, pl.ds(1, 3), cc, rows_of(j)]

    def near(j, k, cc):
        return pltpu.make_async_remote_copy(
            at(yo, yst, j).at[k, cc], dst(y, core, j), ys_s.at[k, cc, sj(j)], ys_r.at[k, core, sj(j)],
            device_id=dev(yd[k], x, cc), device_id_type=MESH)

    def sibling(j):
        return pltpu.make_async_remote_copy(
            at(yo, yst, j).at[0, 1 - core], dst(y, core, j), ys_s.at[0, 1, sj(j)], ys_r.at[0, core, sj(j)],
            device_id=dev(y, x, 1 - core), device_id_type=MESH)

    def local(j):
        return pltpu.make_async_copy(at(yo, yst, j).at[0, core], dst(y, core, j), loc_s.at[sj(j)])

    def hop(j):
        return pltpu.make_async_remote_copy(
            at(yo, yst, j).at[2], at(ro, rb, j), rb_s.at[sj(j)], rb_r.at[sj(j)],
            device_id=dev(yf_, x, core), device_id_type=MESH)

    def forward(j, cc):
        return pltpu.make_async_remote_copy(
            at(ro, rb, j).at[cc], dst(yb_, core, j), fw_s.at[cc, sj(j)], ys_r.at[2, core, sj(j)],
            device_id=dev(yf_, x, cc), device_id_type=MESH)

    def pass_on(j):
        hop(j).wait_recv()
        forward(j, 0).start()
        forward(j, 1).start()

    def project(j, lhs, cosv, sinv, after_hop):
        for k in (2, 1, 3, 0):
            acc = jnp.dot(lhs, w[yd[k]], preferred_element_type=F32)
            for cc in range(2):
                for c in range(3):
                    v = acc[:, (cc * 3 + c) * 128:(cc * 3 + c + 1) * 128]
                    if c < 2:
                        v = v * cosv + pltpu.roll(v, 64, 1) * sinv
                    v = v.astype(BF)
                    if j is None:
                        yo[k, cc, c] = v
                    else:
                        yst[j, k, cc, c] = v.reshape(3, r, 128)
            if k == 2:
                hop(j).start()
            if k == 1:
                near(j, 1, 0).start()
                near(j, 1, 1).start()
                after_hop()
            elif k == 0:
                sibling(j).start()
                local(j).start()
            elif k == 3:
                near(j, k, 0).start()
                near(j, k, 1).start()

    project(None, xo[...], *turn(x, 0, t), lambda: None)

    def step(j, _):
        @pl.when(j + 1 < nc)
        def _():
            own(j + 1, 0).wait_recv()
            relay(j + 1).start()

        @pl.when(j + ahead < nc)
        def _():
            own(j + ahead, 0).start()
            own(j + ahead, 1).start()

        cs = [turn(xs, j * r, r) for xs in xslot]
        cosv = jnp.concatenate([u[0] for u in cs], axis=0)
        sinv = jnp.concatenate([u[1] for u in cs], axis=0)
        own(j, 1).wait_recv()
        relay(j).wait_recv()
        lhs = xg[j].reshape(3 * r, d)

        def after_hop():
            @pl.when(j == 0)
            def _():
                pass_on(None)

            @pl.when(j > 0)
            def _():
                pass_on(j - 1)

        project(j, lhs, cosv, sinv, after_hop)
        return 0

    lax.fori_loop(0, nc, step, 0)
    pass_on(nc - 1)

    def finish(j):
        hop(j).wait_send()
        for cc in range(2):
            forward(j, cc).wait_send()
            for k in (1, 3):
                near(j, k, cc).wait_send()
        sibling(j).wait_send()
        local(j).wait()
        for k in (1, 2, 3):
            for cc in range(2):
                pltpu.make_async_remote_copy(
                    at(yo, yst, j).at[k, cc], dst(yd[n - k], cc, j), ys_s.at[k, cc, sj(j)], ys_r.at[k, cc, sj(j)],
                    device_id=dev(y, x, 1 - core), device_id_type=MESH).wait_recv()
        pltpu.make_async_remote_copy(
            at(yo, yst, j).at[0, core], dst(y, 1 - core, j), ys_s.at[0, 1, sj(j)], ys_r.at[0, 1 - core, sj(j)],
            device_id=dev(y, x, 1 - core), device_id_type=MESH).wait_recv()

    finish(None)

    def drain(j, _):
        for k in range(2):
            own(j, k).wait_send()
        relay(j).wait_send()
        finish(j)
        return 0

    lax.fori_loop(0, nc, drain, 0)


def qkv_exchange(n, nc, ahead, x, g, wqkv):
    t, d = x.shape
    h, dh = wqkv.shape[2:]
    r = t // nc
    dk = 128
    inv = 10000.0 ** (-jnp.arange(dh // 2, dtype=F32) * 2.0 / dh)
    inv = jnp.concatenate([inv, inv]).reshape(1, dh)
    vm = pl.BlockSpec(memory_space=pltpu.VMEM)
    dma = pltpu.SemaphoreType.DMA
    return pl.pallas_call(
        functools.partial(_qkv_kernel, n, nc, ahead),
        out_shape=jax.ShapeDtypeStruct((3, n, 4, 2, t, dh), BF),
        in_specs=[vm, vm, vm, pl.BlockSpec(memory_space=pl.ANY)],
        out_specs=pl.BlockSpec(memory_space=pl.ANY),
        scratch_shapes=[
            pltpu.VMEM((t, d), BF),
            pltpu.VMEM((nc, 3, r, d), BF),
            pltpu.VMEM((6, dk, 3, 2 * n, dh), BF),
            pltpu.VMEM((n, d, 6 * dh), BF),
            pltpu.VMEM((n, 2, 3, t, dh), BF),
            pltpu.VMEM((nc, n, 2, 3, 3, r, dh), BF),
            pltpu.VMEM((2, 3, t, dh), BF),
            pltpu.VMEM((nc, 2, 3, 3, r, dh), BF),
            dma((6,)), dma((2, nc)), dma((3, nc)), dma((nc,)),
            dma((n, 2, nc + 1)), dma((n, 2, nc + 1)), dma((nc + 1,)), dma((nc + 1,)), dma((2, nc + 1)), dma((nc + 1,)),
        ],
        compiler_params=pltpu.CompilerParams(collective_id=0, has_side_effects=True, vmem_limit_bytes=64 * 2**20 - 2**16),
        cost_estimate=pl.CostEstimate(flops=2 * t * d * 3 * h * dh, bytes_accessed=40 * 2**20, transcendentals=0),
    )(x, g.reshape(1, d), inv, wqkv)


NEG = -1e30


def _attn_kernel(n, qt, sub, cw, psub, qkv_ref, x_ref, wo_ref, y_ref,
                 qkv, xv, wo, ob, acc, yacc, vt, qtr, sa, sb, m, ma, mb, insem, wosem, osem, rsem):
    q, k, v = qkv.at[0], qkv.at[1], qkv.at[2]
    s_len, d = k.shape
    bk = qt
    t = ob.shape[0]
    dv = vt.shape[0]
    p = s_len // t
    groups = s_len // qt
    per = qt // t
    c = (d ** -0.5) * math.log2(math.e)
    me = lax.axis_index("seq")
    y, x, core, _ = _place(n)
    head = (x * n + y) * 2 + core
    rot = head // (p // groups)
    my_tile = me // per

    def dev_head(h):
        return (lax.rem(h // 2, n) * n + h // (2 * n)) * 2 + lax.rem(h, 2)

    barrier = pltpu.get_barrier_semaphore()

    def greet(i, _):
        pl.semaphore_signal(barrier, inc=1, device_id={"seq": lax.rem(me + i, p)}, device_id_type=MESH)
        return 0

    lax.fori_loop(1, p, greet, 0)
    for yy in range(n):
        for slot in range(4):
            for cc in range(2):
                off = (0, 2 * cc - 1, 1 - 2 * cc, 2)[slot]
                row = ((yy * n + lax.rem(x + off + n, n)) * 2 + cc) * t
                pltpu.make_async_copy(qkv_ref.at[:, yy, slot, cc], qkv.at[:, pl.ds(pl.multiple_of(row, t), t), :],
                                      insem.at[0]).start()
    pltpu.make_async_copy(x_ref, xv, insem.at[1]).start()
    kw = wo.shape[0] // groups

    def wload(g):
        rows = pl.ds(pl.multiple_of(g * kw, kw), kw)
        return pltpu.make_async_copy(wo_ref.at[rows, :], wo.at[rows, :], wosem.at[g])

    for g in range(groups):
        wload(g).start()
    vt[d:, :] = jnp.ones((dv - d, s_len), BF)
    pltpu.make_async_copy(qkv, qkv, insem.at[0]).wait()

    def tr(j, _):
        blk = pl.ds(pl.multiple_of(j * 512, 512), 512)
        vt[0:d, blk] = v[blk, :].T
        return 0

    lax.fori_loop(0, s_len // 512, tr, 0)

    def qk(j, s_ref, mm, diag=False):
        mx = [None] * (qt // cw)
        for u in range(bk // sub):
            ks = pl.ds(pl.multiple_of(j * bk + u * sub, sub), sub)
            c0 = (u * sub) // cw * cw if diag else 0
            s = jnp.dot(k[ks, :], qtr[:, c0:], preferred_element_type=F32)
            for h in range(c0 // cw, qt // cw):
                sh = s[:, h * cw - c0:(h + 1) * cw - c0]
                if diag and u * sub + sub > h * cw:
                    kp = lax.broadcasted_iota(jnp.int32, sh.shape, 0) + u * sub
                    qp = lax.broadcasted_iota(jnp.int32, sh.shape, 1) + h * cw
                    sh = jnp.where(kp <= qp, sh, NEG)
                s_ref[u * sub:(u + 1) * sub, h * cw:(h + 1) * cw] = sh
                sm = jnp.max(sh, axis=0, keepdims=True)
                mx[h] = sm if mx[h] is None else jnp.maximum(mx[h], sm)
        for h in range(qt // cw):
            mm[:, h * cw:(h + 1) * cw] = mx[h]

    def pv(j, s_ref, mm, diag=False):
        for h in range(qt // cw):
            cols = slice(h * cw, (h + 1) * cw)
            m_old = m[:, cols]
            m_new = jnp.maximum(m_old, mm[:, cols])
            a = jnp.exp2((m_old - m_new) * c)
            mc = m_new * c
            part = None
            for u in range(((h + 1) * cw if diag else bk) // psub):
                ks = pl.ds(pl.multiple_of(j * bk + u * psub, psub), psub)
                pr = jnp.exp2(s_ref[u * psub:(u + 1) * psub, cols] * c - mc)
                dd = jnp.dot(vt[:, ks], pr.astype(BF), preferred_element_type=F32)
                part = dd if part is None else part + dd
            m[:, cols] = m_new
            acc[:, cols] = acc[:, cols] * a + part

    def send(tile, e):
        to = tile * per + e
        return pltpu.make_async_remote_copy(
            v.at[pl.ds(pl.multiple_of(tile * qt + e * t, t), t), :], ob.at[:, pl.ds(pl.multiple_of(head * d, d), d)],
            osem.at[tile, e], rsem.at[head], device_id={"seq": to}, device_id_type=MESH)

    def keep(tile, e):
        return pltpu.make_async_copy(
            v.at[pl.ds(pl.multiple_of(tile * qt + e * t, t), t), :], ob.at[:, pl.ds(pl.multiple_of(head * d, d), d)], osem.at[tile, e])

    def tile_body(i, _):
        tile = lax.rem(i + rot, groups)
        rows = pl.ds(pl.multiple_of(tile * qt, qt), qt)
        qtr[...] = q[rows, :].T
        acc[...] = jnp.zeros_like(acc)
        m[...] = jnp.full_like(m, NEG)
        last = tile

        @pl.when(last == 0)
        def _():
            qk(0, sa, ma, True)
            pv(0, sa, ma, True)

        @pl.when(last > 0)
        def _():
            qk(0, sa, ma)

            def pair(jj, _):
                qk(2 * jj + 1, sb, mb)
                pv(2 * jj, sa, ma)
                qk(2 * jj + 2, sa, ma)
                pv(2 * jj + 1, sb, mb)
                return 0

            npair = (last - 1) // 2
            lax.fori_loop(0, npair, pair, 0)
            b0 = 2 * npair

            @pl.when(last - b0 == 1)
            def _():
                qk(last, sb, mb, True)
                pv(b0, sa, ma)
                pv(last, sb, mb, True)

            @pl.when(last - b0 == 2)
            def _():
                qk(b0 + 1, sb, mb)
                pv(b0, sa, ma)
                qk(last, sa, ma, True)
                pv(b0 + 1, sb, mb)
                pv(last, sa, ma, True)

        o = acc[0:d, :] * (1.0 / acc[d:d + 1, :])
        v[rows, :] = o.T.astype(BF)

        @pl.when(i == 0)
        def _():
            pl.semaphore_wait(barrier, p - 1)

        for e in range(per):
            @pl.when(tile * per + e == me)
            def _():
                keep(tile, e).start()

            @pl.when(tile * per + e != me)
            def _():
                send(tile, e).start()
        return 0

    lax.fori_loop(0, groups, tile_body, 0)
    pltpu.make_async_copy(x_ref, xv, insem.at[1]).wait()
    hp = p // groups
    cw = 1024

    def arrive(h):
        @pl.when(h == head)
        def _():
            keep(my_tile, lax.rem(me, per)).wait()

        @pl.when(h != head)
        def _():
            pltpu.make_async_remote_copy(
                v.at[pl.ds(0, t), :], ob.at[:, pl.ds(pl.multiple_of(h * d, d), d)],
                osem.at[0, 0], rsem.at[h], device_id={"seq": dev_head(h)}, device_id_type=MESH).wait_recv()

    def project(i, _):
        g = lax.rem(my_tile - i + groups, groups)
        wload(g).wait()
        for e in range(hp):
            arrive(g * hp + e)
        o = ob[:, pl.ds(pl.multiple_of(g * kw, kw), kw)]

        def cols(j, _):
            cs = pl.ds(pl.multiple_of(j * cw, cw), cw)
            dd = jnp.dot(o, wo[pl.ds(pl.multiple_of(g * kw, kw), kw), cs], preferred_element_type=F32)

            @pl.when(i == 0)
            def _():
                yacc[:, cs] = xv[:, cs].astype(F32) + dd

            @pl.when(jnp.logical_and(i > 0, i < groups - 1))
            def _():
                yacc[:, cs] = yacc[:, cs] + dd

            @pl.when(i == groups - 1)
            def _():
                y_ref[:, cs] = (yacc[:, cs] + dd).astype(BF)
            return 0

        lax.fori_loop(0, wo.shape[1] // cw, cols, 0)
        return 0

    lax.fori_loop(0, groups, project, 0)

    def drain(tile, _):
        for e in range(per):
            @pl.when(tile * per + e != me)
            def _():
                send(tile, e).wait_send()
        return 0

    lax.fori_loop(0, groups, drain, 0)


def attend(n, qt, sub, cw, psub, qkv, x, wo):
    t, dm = x.shape
    hd = wo.shape[0]
    d = qkv.shape[-1]
    p = 2 * n * n
    s_len = p * t
    groups = s_len // qt
    any_ = pl.BlockSpec(memory_space=pl.ANY)
    dma = pltpu.SemaphoreType.DMA

    return pl.pallas_call(
        functools.partial(_attn_kernel, n, qt, sub, cw, psub),
        out_shape=jax.ShapeDtypeStruct((t, dm), BF),
        in_specs=[any_, any_, any_],
        out_specs=pl.BlockSpec(memory_space=pltpu.VMEM),
        scratch_shapes=[
            pltpu.VMEM((3, s_len, d), BF),
            pltpu.VMEM((t, dm), BF), pltpu.VMEM((hd, dm), BF), pltpu.VMEM((t, hd), BF),
            pltpu.VMEM((d + 16, qt), F32), pltpu.VMEM((t, dm), F32),
            pltpu.VMEM((d + 16, s_len), BF), pltpu.VMEM((d, qt), BF),
            pltpu.VMEM((qt, qt), F32), pltpu.VMEM((qt, qt), F32),
            pltpu.VMEM((1, qt), F32), pltpu.VMEM((1, qt), F32), pltpu.VMEM((1, qt), F32),
            dma((4,)), dma((groups,)), dma((groups, qt // t)), dma((p,)),
        ],
        compiler_params=pltpu.CompilerParams(collective_id=1, has_side_effects=True, vmem_limit_bytes=64 * 2**20 - 2**16),
        cost_estimate=pl.CostEstimate(flops=2 * s_len * s_len * d + 2 * t * hd * dm, bytes_accessed=2 * hd * dm, transcendentals=s_len * s_len // 2),
    )(qkv, x, wo)


def solution(mesh):
    p = mesh.shape["seq"]
    n = math.isqrt(p // 2)
    rows = P(("data", "seq"), None)
    chunks, ahead = 8, 3

    def local(x, g, wqkv, wo):
        t, d = x.shape
        h, dh = wqkv.shape[2:]
        qkv = qkv_exchange(n, chunks, ahead, x, g, wqkv)
        return attend(n, 1024, 512, 256, 256, qkv, x, wo.reshape(h * dh, d))

    return jax.shard_map(local, mesh=mesh,
                         in_specs=(rows, P(None), P(None, None, None, None), P(None, None, None)),
                         out_specs=rows, check_vma=False)
```
